256 devices in a mesh: row: 4 (over x), col: 4 (over y), depth: 16 (over z, core).
Axes of the slice: x: 4, y: 4, z: 8, core: 2. Of those that a mesh axis runs over, the one named last changes fastest.
Arguments:
- tokens: bfloat16 [4096, 4096], P(('col', 'depth'), 'row'), may hold values from -6 to 6
- w_gate: bfloat16 [4096, 14336], P('row', 'col'), may hold values from -0.09375 to 0.09375
- w_up: bfloat16 [4096, 14336], P('row', 'col'), may hold values from -0.09375 to 0.09375
- w_down: bfloat16 [14336, 4096], P('col', 'row'), may hold values from -0.046875 to 0.046875
- cotangent: bfloat16 [4096, 4096], P(('col', 'depth'), 'row'), may hold values from -0.09375 to 0.09375
Outputs:
- mixed: bfloat16 [4096, 4096], P(('col', 'depth'), 'row')
- grad_gate: bfloat16 [4096, 14336], P(('row', 'depth'), 'col')
- grad_up: bfloat16 [4096, 14336], P(('row', 'depth'), 'col')
- grad_down: bfloat16 [14336, 4096], P(('col', 'depth'), 'row')
The draws below stay inside these ranges and needn't reach their ends.
All inputs are finite; a program needn't handle non-finite values.
Results may differ from the reference program's by a relative error of at most 0.025.
Values may be sent and summed in bfloat16 or wider, within the bound.
A program may use at most 128 MiB of HBM per device.

```python
import jax
import jax.numpy as jnp
from jax import lax

D = 4096
FF = 14336
TOK_DEV = 64
TOKENS = 4096
N_ROW = 4
N_COL = 4
N_DEPTH = 16


def steps_of(own_key, shape, pieces, low, top_value):
    level, own = 1.0, jax.random.fold_in(own_key, 6)
    for axis_at, parts in pieces:
        draws = jnp.exp(jax.random.uniform(jax.random.fold_in(own, axis_at), (parts,), jnp.float32, low / len(pieces), top_value / len(pieces)))
        level = level * jnp.repeat(draws, shape[axis_at] // parts).reshape([-1 if axis == axis_at else 1 for axis in range(len(shape))])
    return level


def noise(stream_key, shape, width, reach, split=(), kind=jnp.bfloat16):
    gain = steps_of(stream_key, shape, split, -0.22, 0.18) if split else 1.0
    values = jax.random.normal(stream_key, shape, jnp.float32) * width * gain
    return jnp.minimum(jnp.maximum(values, -reach), reach).astype(kind)


def setup_inputs(seed: int = 0) -> dict:
    splits = jax.random.split(jax.random.key(seed), 6)
    tokens = noise(splits[0], (TOKENS, D), 1.0, 6.0, ((0, 64), (1, 4)))
    w_gate = noise(splits[1], (D, FF), D ** -0.5, 0.09375, ((0, 4), (1, 4)))
    w_up = noise(splits[2], (D, FF), D ** -0.5, 0.09375, ((0, 4), (1, 4)))
    w_down = noise(splits[3], (FF, D), FF ** -0.5, 0.046875, ((0, 4), (1, 4)))
    cotangent = noise(splits[4], (TOKENS, D), (TOKENS ** -0.5), 0.09375, ((0, 64), (1, 4)))
    return dict(tokens=tokens, w_gate=w_gate, w_up=w_up, w_down=w_down, cotangent=cotangent)


COLS_CONTRACT = (((1,), (1,)), ((), ()))
ROWS_CONTRACT = (((0,), (0,)), ((), ()))


def rounded_add(running, addend):
    rounded = lax.optimization_barrier(addend.astype(jnp.bfloat16))
    return running + rounded.astype(jnp.float32)


def layer_rows(array, layer_index):
    shaped = array.reshape(N_COL, N_DEPTH, TOK_DEV, array.shape[1])
    return shaped[:, layer_index].reshape(N_COL * TOK_DEV, array.shape[1])


def reference(tokens, w_gate, w_up, w_down, cotangent):
    feat_width = D // N_ROW
    token_count = tokens.shape[0]
    gate_sum = jnp.zeros((token_count, FF), jnp.float32)
    up_sum = jnp.zeros((token_count, FF), jnp.float32)
    hidden_grad = jnp.zeros((token_count, FF), jnp.float32)
    for block_index in range(N_ROW):
        lower_edge = block_index * feat_width
        upper_edge = lower_edge + feat_width
        tok_block = tokens[:, lower_edge:upper_edge]
        gate_sum = rounded_add(gate_sum, jnp.dot(tok_block, w_gate[lower_edge:upper_edge], preferred_element_type=jnp.float32))
        up_sum = rounded_add(up_sum, jnp.dot(tok_block, w_up[lower_edge:upper_edge], preferred_element_type=jnp.float32))
        hidden_grad = rounded_add(hidden_grad, lax.dot_general(cotangent[:, lower_edge:upper_edge], w_down[:, lower_edge:upper_edge], COLS_CONTRACT, preferred_element_type=jnp.float32))
    hidden = (jax.nn.silu(gate_sum) * up_sum).astype(jnp.bfloat16)
    mixed = jnp.dot(hidden, w_down, preferred_element_type=jnp.float32).astype(jnp.bfloat16)
    sigmoid_gate = jax.nn.sigmoid(gate_sum)
    d_gate = (hidden_grad * up_sum * sigmoid_gate * (1.0 + gate_sum * (1.0 - sigmoid_gate))).astype(jnp.bfloat16)
    d_up = (hidden_grad * gate_sum * sigmoid_gate).astype(jnp.bfloat16)
    grad_gate = jnp.zeros((D, FF), jnp.float32)
    grad_up = jnp.zeros((D, FF), jnp.float32)
    grad_down = jnp.zeros((FF, D), jnp.float32)
    for layer_index in range(N_DEPTH):
        tok_layer = layer_rows(tokens, layer_index)
        grad_gate = rounded_add(grad_gate, lax.dot_general(tok_layer, layer_rows(d_gate, layer_index), ROWS_CONTRACT, preferred_element_type=jnp.float32))
        grad_up = rounded_add(grad_up, lax.dot_general(tok_layer, layer_rows(d_up, layer_index), ROWS_CONTRACT, preferred_element_type=jnp.float32))
        grad_down = rounded_add(grad_down, lax.dot_general(layer_rows(hidden, layer_index), layer_rows(cotangent, layer_index), ROWS_CONTRACT, preferred_element_type=jnp.float32))
    return (mixed, grad_gate.astype(jnp.bfloat16), grad_up.astype(jnp.bfloat16), grad_down.astype(jnp.bfloat16))
```

```python
import jax
import jax.numpy as jnp
from jax import lax
from jax.experimental import pallas as pl
from jax.experimental.pallas import tpu as pltpu
from jax.sharding import PartitionSpec as P

MESH = pl.DeviceIdType.MESH
BF, F32 = jnp.bfloat16, jnp.float32
TD, FW, HW = 64, 1024, 3584
NY, NZ = 4, 8
CW = 128
HC = HW // 2
NC = HC // CW
TK = 2 * NY * TD
OW = TK // 4
HF = OW // 2
PIECE = HC // 8
SL, PS = 4, 6

TICK = {"A": 0, "RS2": 1, "AG1": 2, "AG2": 3, "E": 4, "Z1": 6, "Z2": 7, "Z3": 8, "Z4": 9, "Z5": 10, "Z6": 11, "FIN": 12}
ORDER = ["FIN", "Z6", "Z5", "Z4", "Z3", "Z2", "Z1", "AG2", "AG1", "RS2", "A", "E"]


def remote(src, dst, ssem, rsem, **dev):
    return pltpu.make_async_remote_copy(
        src_ref=src, dst_ref=dst, send_sem=ssem, recv_sem=rsem, device_id=dev, device_id_type=MESH
    )


def mod(a, n):
    return lax.rem(a + n, n)


def rows(start, size):
    return pl.ds(pl.multiple_of(start, size), size)


def kernel(
    tok, wg, wu, wd, cot, o_mix, o_gate, o_up, o_down,
    T, C, TT, CT, WGU, WD, PX, R1, R2, G, PZ, ZB, ACC, XS, OGU, GDT, OGD, MS, MR, MYS, MYR, OM,
    s_in, s_w, s_ag, r_ag, s_fw, s_x1, r_x1, s_x2, r_x2, s_g1, r_g1, s_g2, r_g2, s_z, r_z,
    s_xs, r_xs, s_gd, r_gd, s_m, r_m, s_my, r_my, s_out,
):
    r, y, d = lax.axis_index("row"), lax.axis_index("col"), lax.axis_index("depth")
    z, k = lax.div(d, 2), lax.rem(d, 2)
    right, left = mod(r + 1, 4), mod(r + 3, 4)
    opp = mod(r + 2, 4)
    zup = 2 * mod(z + 1, NZ) + k
    zdn = 2 * mod(z + NZ - 1, NZ) + k
    mate = 2 * z + (1 - k)
    own = 4 * k + y

    in_t = pltpu.make_async_copy(tok, T.at[rows(own * TD, TD), :], s_in.at[0])
    in_c = pltpu.make_async_copy(cot, C.at[rows(own * TD, TD), :], s_in.at[1])
    in_t.start()
    in_c.start()

    def weight_copies(j):
        at = pl.ds(pl.multiple_of(k * HC + j * CW, CW), CW)
        return (
            pltpu.make_async_copy(wg.at[:, at], WGU.at[j, :, pl.ds(0, CW)], s_w.at[0, j]),
            pltpu.make_async_copy(wu.at[:, at], WGU.at[j, :, pl.ds(CW, CW)], s_w.at[1, j]),
            pltpu.make_async_copy(wd.at[at, :], WD.at[j], s_w.at[2, j]),
        )

    barrier = pltpu.get_barrier_semaphore()
    for other in (right, left):
        pl.semaphore_signal(barrier, inc=1, device_id={"row": other}, device_id_type=MESH)
    for dy in range(1, 4):
        pl.semaphore_signal(barrier, inc=1, device_id={"col": mod(y + dy, 4)}, device_id_type=MESH)
    for dd in range(1, 16):
        pl.semaphore_signal(barrier, inc=1, device_id={"depth": mod(d + dd, 16)}, device_id_type=MESH)

    @pl.loop(0, NC)
    def _(j):
        for c in weight_copies(j):
            c.start()

    ACC[...] = jnp.zeros_like(ACC)
    pl.semaphore_wait(barrier, 20)

    def block_of(a, b):
        return (T, C)[a].at[rows(b * TD, TD), :]

    for a, mine in ((0, in_t), (1, in_c)):
        mine.wait()
        for dy in (1, 3, 2):
            remote(block_of(a, own), block_of(a, own), s_ag.at[a, dy], r_ag.at[a, own], col=mod(y + dy, 4)).start()
        remote(block_of(a, own), block_of(a, own), s_ag.at[a, 0], r_ag.at[a, own], depth=mate).start()
    for a in (0, 1):
        for dy in (1, 3, 2):
            b = 4 * k + mod(y + dy, 4)
            remote(block_of(a, b), block_of(a, b), s_fw.at[a, dy - 1], r_ag.at[a, b], depth=mate).wait_recv()
            remote(block_of(a, b), block_of(a, b), s_fw.at[a, dy - 1], r_ag.at[a, b], depth=mate).start()
    for a in (0, 1):
        for yy in range(4):
            b = 4 * (1 - k) + yy
            remote(block_of(a, b), block_of(a, b), s_fw.at[a, 0], r_ag.at[a, b], depth=mate).wait_recv()
    for a in (0, 1):
        for dy in range(4):
            remote(block_of(a, own), block_of(a, own), s_ag.at[a, dy], r_ag.at[a, own], depth=mate).wait_send()
        for dy in (1, 3, 2):
            b = 4 * k + mod(y + dy, 4)
            remote(block_of(a, b), block_of(a, b), s_fw.at[a, dy - 1], r_ag.at[a, b], depth=mate).wait_send()

    def xto(di):
        return {"row": (right, left)[di]}

    def x1_copy(j, di):
        sl = lax.rem(j, SL)
        src = PX.at[sl, :, rows(opp * OW + di * HF, HF), :]
        return remote(src, R1.at[sl, di], s_x1.at[di, sl], r_x1.at[di, sl], **xto(di))

    def x2_copy(j, di):
        sl = lax.rem(j, SL)
        src = PX.at[sl, :, rows((right, left)[di] * OW, OW), :]
        return remote(src, R2.at[sl, di], s_x2.at[di, sl], r_x2.at[di, sl], **xto(di))

    def g1_copy(j, di, owner):
        sl = lax.rem(j, SL)
        at = G.at[sl, :, rows(owner * OW, OW), :]
        return remote(at, at, s_g1.at[di, sl], r_g1.at[di, sl], **xto(di))

    def g2_copy(j, di, owner):
        sl = lax.rem(j, SL)
        at = G.at[sl, :, rows(owner * OW + di * HF, HF), :]
        return remote(at, at, s_g2.at[di, sl], r_g2.at[di, sl], **xto(di))

    def zrow(di, s):
        q = mod(z - 1 - s + NZ, NZ) if di == 0 else mod(z + 1 + s, NZ)
        return rows(q * 128 + di * 64, 64)

    def z_copy(j, di, s):
        sl = lax.rem(j, SL)
        if s == 0:
            src = PZ.at[lax.rem(j, PS), :, zrow(di, 0), :]
        else:
            src = ZB.at[di, s - 1, sl]
        return remote(src, ZB.at[di, s, sl], s_z.at[di, s, sl], r_z.at[di, s, sl], depth=(zup, zdn)[di])

    def stage_a(j):
        sl = lax.rem(j, SL)
        for c in weight_copies(j):
            c.wait()
        for m in range(2):
            at = pl.ds(m * 256, 256)
            gu = jnp.dot(T[at, :], WGU[j], preferred_element_type=F32)
            h = lax.dot_general(C[at, :], WD[j], (((1,), (1,)), ((), ())), preferred_element_type=F32)
            PX[sl, 0, at, :] = gu[:, :CW].astype(BF)
            PX[sl, 1, at, :] = gu[:, CW:].astype(BF)
            PX[sl, 2, at, :] = h.astype(BF)
        for di in (0, 1):
            x1_copy(j, di).start()

    def stage_rs2(j):
        sl = lax.rem(j, SL)
        for di in (0, 1):
            x1_copy(j, di).wait_recv()
            at = rows((right, left)[di] * OW + di * HF, HF)
            PX[sl, :, at, :] = (PX[sl, :, at, :].astype(F32) + R1[sl, di].astype(F32)).astype(BF)
            x2_copy(j, di).start()

    def stage_ag1(j):
        sl = lax.rem(j, SL)
        for di in (0, 1):
            x1_copy(j, di).wait_send()
        for di in (0, 1):
            x2_copy(j, di).wait_recv()
        at = rows(r * OW, OW)
        total = PX[sl, :, at, :].astype(F32) + R2[sl, 0].astype(F32) + R2[sl, 1].astype(F32)
        gate, up, hg = total[0], total[1], total[2]
        sig = jax.nn.sigmoid(gate)
        G[sl, 0, at, :] = (gate * sig * up).astype(BF)
        G[sl, 1, at, :] = (hg * up * sig * (1.0 + gate * (1.0 - sig))).astype(BF)
        G[sl, 2, at, :] = (hg * gate * sig).astype(BF)
        for di in (0, 1):
            g1_copy(j, di, r).start()

    def stage_ag2(j):
        for di in (0, 1):
            frm = (left, right)[di]
            g1_copy(j, di, frm).wait_recv()
            g2_copy(j, di, frm).start()

    def stage_e(j):
        sl, ps = lax.rem(j, SL), lax.rem(j, PS)
        for di in (0, 1):
            x2_copy(j, di).wait_send()
            g1_copy(j, di, r).wait_send()
        for di in (0, 1):
            g2_copy(j, di, opp).wait_recv()
        hid = G[sl, 0]
        dgu = jnp.concatenate([G[sl, 1], G[sl, 2]], axis=1)
        for m in range(4):
            at = pl.ds(m * 256, 256)
            gu = jnp.dot(TT[at, :], dgu, preferred_element_type=F32)
            PZ[ps, 0, at, :] = gu[:, :CW].astype(BF)
            PZ[ps, 1, at, :] = gu[:, CW:].astype(BF)
            PZ[ps, 2, at, :] = jnp.dot(CT[at, :], hid, preferred_element_type=F32).astype(BF)
        for di in (0, 1):
            z_copy(j, di, 0).start()
        for m in range(4):
            at = pl.ds(m * 128, 128)
            ACC[at, :] += jnp.dot(G[sl, 0, at, :], WD[j], preferred_element_type=F32)

    def stage_z(s):
        def run(j):
            sl, ps = lax.rem(j, SL), lax.rem(j, PS)
            if s == 1:
                for di in (0, 1):
                    g2_copy(j, di, (left, right)[di]).wait_send()
            else:
                for di in (0, 1):
                    z_copy(j, di, s - 2).wait_send()
            for di in (0, 1):
                z_copy(j, di, s - 1).wait_recv()
                part = PZ[ps, :, zrow(di, s), :].astype(F32)
                ZB[di, s - 1, sl] = (ZB[di, s - 1, sl].astype(F32) + part).astype(BF)
                z_copy(j, di, s).start()

        return run

    def swap_copy(j):
        at = OGU.at[:, :, pl.ds(pl.multiple_of(k * HC + j * CW, CW), CW)]
        return remote(XS.at[j], at, s_xs.at[j], r_xs.at[j], depth=mate)

    def swap_in(j):
        at = OGU.at[:, :, pl.ds(pl.multiple_of((1 - k) * HC + j * CW, CW), CW)]
        return remote(XS.at[j], at, s_xs.at[j], r_xs.at[j], depth=mate)

    def piece_src(m):
        return GDT.at[rows(m * PIECE, 32) if False else pl.ds(pl.multiple_of(m * PIECE, 32), PIECE), :]

    def piece_dst(zz):
        return OGD.at[:, rows(zz * 128, 128)]

    def piece_copy(m):
        return remote(piece_src(m), piece_dst(z), s_gd.at[m], r_gd.at[z], depth=8 * k + m)

    def piece_local(m):
        return pltpu.make_async_copy(piece_src(m), piece_dst(z), r_gd.at[z])

    def stage_fin(j):
        sl, ps = lax.rem(j, SL), lax.rem(j, PS)
        sums = []
        for di in (0, 1):
            for s in (5, 6):
                z_copy(j, di, s).wait_send()
        for di in (0, 1):
            z_copy(j, di, 6).wait_recv()
            part = PZ[ps, :, rows(z * 128 + di * 64, 64), :].astype(F32)
            sums.append(ZB[di, 6, sl].astype(F32) + part)
        lo, hi = sums
        first = k == 0
        at = pl.ds(pl.multiple_of(k * HC + j * CW, CW), CW)
        OGU[:, :, at] = jnp.where(first, lo[:2], hi[:2]).astype(BF)
        XS[j] = jnp.where(first, hi[:2], lo[:2]).astype(BF)
        swap_copy(j).start()
        down = jnp.concatenate([lo[2], hi[2]], axis=0)
        GDT[rows(j * CW, CW), :] = down.T.astype(BF)
        m = lax.div(4 * j, 7)

        @pl.when(lax.div(4 * (j + 1), 7) > m)
        def _():
            to_self = 8 * k + m == d

            @pl.when(to_self)
            def _():
                piece_local(m).start()

            @pl.when(jnp.logical_not(to_self))
            def _():
                piece_copy(m).start()

    def mate_copy():
        return remote(MS, MR, s_m.at[0], r_m.at[0], depth=mate)

    def col_copy(dy):
        return remote(MYS.at[dy], MYR.at[dy], s_my.at[dy], r_my.at[dy], col=mod(y + dy, 4))

    def mix1():
        MS[...] = ACC[rows((1 - k) * 256, 256), :].astype(BF)
        mate_copy().start()

    def mix2():
        mate_copy().wait()
        for dy in (1, 3, 2):
            yy = mod(y + dy, 4)
            total = ACC[rows(k * 256 + yy * TD, TD), :] + MR[rows(yy * TD, TD), :].astype(F32)
            MYS[dy] = total.astype(BF)
            col_copy(dy).start()

    def mix3():
        total = ACC[rows(k * 256 + y * TD, TD), :] + MR[rows(y * TD, TD), :].astype(F32)
        for dy in (1, 3, 2):
            col_copy(dy).wait()
            total = total + MYR[dy].astype(F32)
        OM[...] = total.astype(BF)
        pltpu.make_async_copy(OM, o_mix, s_out.at[0]).start()

    TT[...] = T[...].T
    CT[...] = C[...].T

    stages = {"A": stage_a, "RS2": stage_rs2, "AG1": stage_ag1, "AG2": stage_ag2, "E": stage_e, "FIN": stage_fin}
    for s in range(1, 7):
        stages[f"Z{s}"] = stage_z(s)
    last_e = NC - 1 + TICK["E"] // 2

    @pl.loop(0, NC + TICK["FIN"] // 2)
    def _(i):
        for parity in (0, 1):
            for name in ORDER:
                if TICK[name] % 2 != parity:
                    continue
                j = i - TICK[name] // 2

                @pl.when(jnp.logical_and(j >= 0, j < NC))
                def _(name=name, j=j):
                    stages[name](j)

            if parity == 1:
                for n, step in enumerate((mix1, mix2, mix3)):
                    pl.when(i == last_e + n)(step)

    outs = []
    for j in range(NC):
        swap_in(j).wait_recv()
    for n, o in ((0, o_gate), (1, o_up)):
        outs.append(pltpu.make_async_copy(OGU.at[n], o, s_out.at[1 + n]))
        outs[-1].start()
    has_self = lax.div(d, 8) == k
    for zz in range(NZ):
        local = jnp.logical_and(has_self, z == zz)

        @pl.when(local)
        def _(zz=zz):
            pltpu.make_async_copy(piece_src(0), piece_dst(zz), r_gd.at[zz]).wait()

        @pl.when(jnp.logical_not(local))
        def _(zz=zz):
            remote(piece_src(0), piece_dst(zz), s_gd.at[0], r_gd.at[zz], depth=mate).wait_recv()

    outs.append(pltpu.make_async_copy(OGD, o_down, s_out.at[3]))
    outs[-1].start()
    for j in range(NC):
        swap_copy(j).wait_send()
    for m in range(8):

        @pl.when(8 * k + m != d)
        def _(m=m):
            piece_copy(m).wait_send()

    pltpu.make_async_copy(OM, o_mix, s_out.at[0]).wait()
    for o in outs:
        o.wait()


def per_device(tokens, w_gate, w_up, w_down, cotangent):
    dma = pltpu.SemaphoreType.DMA
    scratch = [
        pltpu.VMEM((TK, FW), BF),
        pltpu.VMEM((TK, FW), BF),
        pltpu.VMEM((FW, TK), BF),
        pltpu.VMEM((FW, TK), BF),
        pltpu.VMEM((NC, FW, 2 * CW), BF),
        pltpu.VMEM((NC, CW, FW), BF),
        pltpu.VMEM((SL, 3, TK, CW), BF),
        pltpu.VMEM((SL, 2, 3, HF, CW), BF),
        pltpu.VMEM((SL, 2, 3, OW, CW), BF),
        pltpu.VMEM((SL, 3, TK, CW), BF),
        pltpu.VMEM((PS, 3, FW, CW), BF),
        pltpu.VMEM((2, 7, SL, 3, 64, CW), BF),
        pltpu.VMEM((TK, FW), F32),
        pltpu.VMEM((NC, 2, 64, CW), BF),
        pltpu.VMEM((2, 64, HW), BF),
        pltpu.VMEM((HC, 128), BF),
        pltpu.VMEM((PIECE, FW), BF),
        pltpu.VMEM((256, FW), BF),
        pltpu.VMEM((256, FW), BF),
        pltpu.VMEM((4, TD, FW), BF),
        pltpu.VMEM((4, TD, FW), BF),
        pltpu.VMEM((TD, FW), BF),
        dma((2,)), dma((3, NC)),
        dma((2, 4)), dma((2, 8)), dma((2, 3)),
        dma((2, SL)), dma((2, SL)), dma((2, SL)), dma((2, SL)),
        dma((2, SL)), dma((2, SL)), dma((2, SL)), dma((2, SL)),
        dma((2, 7, SL)), dma((2, 7, SL)),
        dma((NC,)), dma((NC,)), dma((8,)), dma((8,)),
        dma((1,)), dma((1,)), dma((4,)), dma((4,)), dma((4,)),
    ]
    anyspec = pl.BlockSpec(memory_space=pl.ANY)
    return pl.pallas_call(
        kernel,
        out_shape=(
            jax.ShapeDtypeStruct((TD, FW), BF),
            jax.ShapeDtypeStruct((FW // 16, HW), BF),
            jax.ShapeDtypeStruct((FW // 16, HW), BF),
            jax.ShapeDtypeStruct((HW // 16, FW), BF),
        ),
        in_specs=[anyspec] * 5,
        out_specs=(anyspec,) * 4,
        scratch_shapes=scratch,
        compiler_params=pltpu.CompilerParams(
            collective_id=0, has_side_effects=True, vmem_limit_bytes=58 * 1024 * 1024
        ),
    )(tokens, w_gate, w_up, w_down, cotangent)


def solution(mesh):
    tok, grad = P(("col", "depth"), "row"), P(("row", "depth"), "col")
    return jax.shard_map(
        per_device,
        mesh=mesh,
        in_specs=(tok, P("row", "col"), P("row", "col"), P("col", "row"), tok),
        out_specs=(tok, grad, grad, P(("col", "depth"), "row")),
        check_vma=False,
    )
```

```python
import jax
import jax.numpy as jnp
from jax import lax
from jax.experimental import pallas as pl
from jax.experimental.pallas import tpu as pltpu
from jax.sharding import PartitionSpec as P

MESH = pl.DeviceIdType.MESH
BF, F32 = jnp.bfloat16, jnp.float32
TD, FW, HW = 64, 1024, 3584
NY, NZ = 4, 8
CW = 128
HC = HW // 2
NC = HC // CW
TK = 2 * NY * TD
OW = TK // 4
HF = OW // 2
SL, ZS, PS = 6, 6, 12
ST = CW // NZ

PT = 3
TICK = {"A": 0, "RS2": 2, "AG1": 5, "AG2": 8, "E": 10, "Z1": 13, "Z2": 15, "Z3": 17, "Z4": 19, "Z5": 21, "Z6": 23, "FIN": 25}
ORDER = ["FIN", "Z6", "Z5", "Z4", "Z3", "Z2", "Z1", "AG2", "AG1", "RS2", "A", "E"]


def remote(src, dst, ssem, rsem, **dev):
    return pltpu.make_async_remote_copy(
        src_ref=src, dst_ref=dst, send_sem=ssem, recv_sem=rsem, device_id=dev, device_id_type=MESH
    )


def mod(a, n):
    return lax.rem(a + n, n)


def rows(start, size):
    return pl.ds(pl.multiple_of(start, size), size)


def kernel(
    tok, wg, wu, wd, cot, o_mix, o_gate, o_up, o_down,
    T, C, TT, WG, WU, WC, WD, PX, R1, R2, G, PZ, ZB, ACC, XS, XR, OGU, OGB, OGD, MS, MR, MYS, MYR, OM,
    s_in, s_w, s_wd, s_ag, r_ag, s_fw, s_rl, r_rl, s_x1, r_x1, s_x2, r_x2, s_g1, r_g1, s_g2, r_g2, s_z, r_z,
    s_xs, r_xs, s_m, r_m, s_my, r_my, s_out,
):
    r, y, d = lax.axis_index("row"), lax.axis_index("col"), lax.axis_index("depth")
    z, k = lax.div(d, 2), lax.rem(d, 2)
    right, left = mod(r + 1, 4), mod(r + 3, 4)
    opp = mod(r + 2, 4)
    zup = 2 * mod(z + 1, NZ) + k
    zdn = 2 * mod(z + NZ - 1, NZ) + k
    mate = 2 * z + (1 - k)
    own = 4 * k + y

    in_t = pltpu.make_async_copy(tok, T.at[rows(own * TD, TD), :], s_in.at[0])
    in_c = pltpu.make_async_copy(cot, C.at[rows(own * TD, TD), :], s_in.at[1])
    in_t.start()
    in_c.start()

    def start_down(j):
        for zz in range(NZ):
            src = wd.at[pl.ds(pl.multiple_of(448 * zz + 224 * k + ST * j, ST), ST), :]
            to = lax.rem(16 * (6 * k + j + 4 * (zz % 2) + zz // 2), CW)
            pltpu.make_async_copy(src, WD.at[j, rows(to, ST), :], s_wd.at[j]).start()

    def wide_copy(n, q):
        at = pl.ds(q * 256, 256)
        return pltpu.make_async_copy((wg, wu)[n].at[at, :], (WG, WU)[n].at[at, :], s_w.at[n])

    barrier = pltpu.get_barrier_semaphore()
    for other in (right, left):
        pl.semaphore_signal(barrier, inc=1, device_id={"row": other}, device_id_type=MESH)
    for dy in range(1, 4):
        pl.semaphore_signal(barrier, inc=1, device_id={"col": mod(y + dy, 4)}, device_id_type=MESH)
    for dd in range(1, 16):
        pl.semaphore_signal(barrier, inc=1, device_id={"depth": mod(d + dd, 16)}, device_id_type=MESH)

    for n in (0, 1):
        for q in range(4):
            wide_copy(n, q).start()
    pl.loop(0, NC)(start_down)
    ACC[...] = jnp.zeros_like(ACC)
    pl.semaphore_wait(barrier, 20)

    def block_of(a, b):
        return (T, C)[a].at[rows(b * TD, TD), :]

    yto = (mod(y + 1, 4), mod(y + 3, 4))
    yop = 4 * k + mod(y + 2, 4)

    def own_copy(a, di):
        dev = {"depth": mate} if di == 2 else {"col": yto[di]}
        return remote(block_of(a, own), block_of(a, own), s_ag.at[a, di], r_ag.at[a, own], **dev)

    def relay_copy(a, di, b):
        at = (T, C)[a].at[rows(b * TD + di * (TD // 2), TD // 2), :]
        return remote(at, at, s_rl.at[a, di], r_rl.at[a, di], col=yto[di])

    def mate_block(a, n, b):
        return remote(block_of(a, b), block_of(a, b), s_fw.at[a, n], r_ag.at[a, b], depth=mate)

    for a, mine in ((0, in_t), (1, in_c)):
        mine.wait()
        for di in range(3):
            own_copy(a, di).start()
    for a in (0, 1):
        for di in (0, 1):
            b = 4 * k + yto[1 - di]
            mate_block(a, di, b).wait_recv()
            relay_copy(a, di, b).start()
            mate_block(a, di, b).start()
    for a in (0, 1):
        for di in (0, 1):
            relay_copy(a, di, yop).wait_recv()
        mate_block(a, 2, yop).start()
    for a in (0, 1):
        for yy in range(4):
            mate_block(a, 0, 4 * (1 - k) + yy).wait_recv()

    def xto(di):
        return {"row": (right, left)[di]}

    def x1_copy(j, di):
        sl = lax.rem(j, SL)
        src = PX.at[sl, :, rows(opp * OW + di * HF, HF), :]
        return remote(src, R1.at[sl, di], s_x1.at[di, sl], r_x1.at[di, sl], **xto(di))

    def x2_copy(j, di):
        sl = lax.rem(j, SL)
        src = PX.at[sl, :, rows((right, left)[di] * OW, OW), :]
        return remote(src, R2.at[sl, di], s_x2.at[di, sl], r_x2.at[di, sl], **xto(di))

    def g1_copy(j, di, owner):
        sl = lax.rem(j, SL)
        at = G.at[sl, :, rows(owner * OW, OW), :]
        return remote(at, at, s_g1.at[di, sl], r_g1.at[di, sl], **xto(di))

    def g2_copy(j, di, owner):
        sl = lax.rem(j, SL)
        at = G.at[sl, :, rows(owner * OW + di * HF, HF), :]
        return remote(at, at, s_g2.at[di, sl], r_g2.at[di, sl], **xto(di))

    def zrow(di, s):
        q = mod(z - 1 - s + NZ, NZ) if di == 0 else mod(z + 1 + s, NZ)
        return rows(q * 128 + di * 64, 64)

    def z_copy(j, di, s):
        sl = lax.rem(j, ZS)
        if s == 0:
            src = PZ.at[lax.rem(j, PS), :, zrow(di, 0), :]
        else:
            src = ZB.at[di, s - 1, sl]
        return remote(src, ZB.at[di, s, sl], s_z.at[di, s, sl], r_z.at[di, s, sl], depth=(zup, zdn)[di])

    def lane_block(kk, j, zz):
        return rows(lax.div(448 * zz + 224 * kk + ST * j, CW) * CW, CW)

    def strip_at(j):
        lane = lax.broadcasted_iota(jnp.int32, (128, CW), 1)
        u = lax.rem(lax.div(lane, ST) + 16 - lax.rem(6 * k + j, 8), 8)
        return 2 * lax.rem(u, 4) + lax.div(u, 4)

    def stage_a(j):
        sl = lax.rem(j, SL)
        pltpu.make_async_copy(wd.at[pl.ds(0, CW), :], WD.at[j], s_wd.at[j]).wait()

        @pl.when(j == 0)
        def _():
            for n, (w, buf) in enumerate(((wg, WG), (wu, WU))):
                pltpu.make_async_copy(w, buf, s_w.at[n]).wait()

        which = strip_at(j)
        for n, buf in enumerate((WG, WU)):
            for q in range(8):
                at = pl.ds(q * 128, 128)
                got = buf[at, lane_block(k, j, 0)]
                for zz in range(1, NZ):
                    part = buf[at, lane_block(k, j, zz)]
                    if zz // 2:
                        part = pltpu.roll(part, ST * (zz // 2), 1)
                    got = jnp.where(which == zz, part, got)
                WC[at, n * CW : (n + 1) * CW] = got
        for m in range(2):
            at = pl.ds(m * 256, 256)
            gu = jnp.dot(T[at, :], WC[...], preferred_element_type=F32)
            h = lax.dot_general(C[at, :], WD[j], (((1,), (1,)), ((), ())), preferred_element_type=F32)
            PX[sl, 0, at, :] = gu[:, :CW].astype(BF)
            PX[sl, 1, at, :] = gu[:, CW:].astype(BF)
            PX[sl, 2, at, :] = h.astype(BF)
        for di in (0, 1):
            x1_copy(j, di).start()

    def stage_rs2(j):
        sl = lax.rem(j, SL)
        for di in (0, 1):
            x1_copy(j, di).wait_recv()
            at = rows((right, left)[di] * OW + di * HF, HF)
            PX[sl, :, at, :] = (PX[sl, :, at, :].astype(F32) + R1[sl, di].astype(F32)).astype(BF)
            x2_copy(j, di).start()

    def stage_ag1(j):
        sl = lax.rem(j, SL)
        for di in (0, 1):
            x1_copy(j, di).wait_send()
        for di in (0, 1):
            x2_copy(j, di).wait_recv()
        at = rows(r * OW, OW)
        total = PX[sl, :, at, :].astype(F32) + R2[sl, 0].astype(F32) + R2[sl, 1].astype(F32)
        gate, up, hg = total[0], total[1], total[2]
        sig = jax.nn.sigmoid(gate)
        G[sl, 0, at, :] = (gate * sig * up).astype(BF)
        G[sl, 1, at, :] = (hg * up * sig * (1.0 + gate * (1.0 - sig))).astype(BF)
        G[sl, 2, at, :] = (hg * gate * sig).astype(BF)
        for di in (0, 1):
            g1_copy(j, di, r).start()

    def stage_ag2(j):
        for di in (0, 1):
            frm = (left, right)[di]
            g1_copy(j, di, frm).wait_recv()
            g2_copy(j, di, frm).start()

    def stage_e(j):
        sl, ps = lax.rem(j, SL), lax.rem(j, PS)
        for di in (0, 1):
            x2_copy(j, di).wait_send()
            g1_copy(j, di, r).wait_send()
        for di in (0, 1):
            g2_copy(j, di, opp).wait_recv()
        hid = G[sl, 0]
        dgu = jnp.concatenate([G[sl, 1], G[sl, 2]], axis=1)
        for m in range(4):
            at = pl.ds(m * 256, 256)
            gu = jnp.dot(TT[at, :], dgu, preferred_element_type=F32)
            PZ[ps, 0, at, :] = gu[:, :CW].astype(BF)
            PZ[ps, 1, at, :] = gu[:, CW:].astype(BF)
        hid_t = hid.T
        for h in range(2):
            down = jnp.dot(hid_t, C[:, h * 512 : h * 512 + 512], preferred_element_type=F32).astype(BF)
            for ub in range(8):
                u = lax.rem(ub + 16 - lax.rem(6 * k + j, 8), 8)
                top = (2 * lax.rem(u, 4) + lax.div(u, 4)) * 128 + h * 64
                for cb in range(4):
                    tile = down[ub * ST : ub * ST + ST, cb * 128 : cb * 128 + 128]
                    PZ[ps, 2, pl.ds(pl.multiple_of(top + cb * ST, ST), ST), :] = tile
        for di in (0, 1):
            z_copy(j, di, 0).start()
        for m in range(4):
            at = pl.ds(m * 128, 128)
            ACC[at, :] += jnp.dot(G[sl, 0, at, :], WD[j], preferred_element_type=F32)

    def stage_z(s):
        def run(j):
            sl, ps = lax.rem(j, ZS), lax.rem(j, PS)
            if s == 1:
                for di in (0, 1):
                    g2_copy(j, di, (left, right)[di]).wait_send()
            else:
                for di in (0, 1):
                    z_copy(j, di, s - 2).wait_send()
            for di in (0, 1):
                z_copy(j, di, s - 1).wait_recv()
                part = PZ[ps, :, zrow(di, s), :].astype(F32)
                ZB[di, s - 1, sl] = (ZB[di, s - 1, sl].astype(F32) + part).astype(BF)
                z_copy(j, di, s).start()

        return run

    def swap_copy(j):
        return remote(XS.at[j], XR.at[j], s_xs.at[j], r_xs.at[j], depth=mate)

    def put(value, kk, j):
        lane = lax.div(lax.broadcasted_iota(jnp.int32, (2, 64, CW), 2), ST)
        for g in range(4):
            turned = pltpu.roll(value, CW - ST * g, 2) if g else value
            for zz in (2 * g, 2 * g + 1):
                at = lane_block(kk, j, zz)
                here = lane == lax.rem(4 * zz + 6 * kk + j, 8)
                OGU[:, :, at] = jnp.where(here, turned, OGU[:, :, at])

    def put_swapped(j):
        swap_copy(j).wait_recv()
        put(XR[j].astype(F32), 1 - k, j)

    def stage_fin(j):
        sl, ps = lax.rem(j, ZS), lax.rem(j, PS)
        sums = []
        for di in (0, 1):
            for s in (5, 6):
                z_copy(j, di, s).wait_send()
        for di in (0, 1):
            z_copy(j, di, 6).wait_recv()
            part = PZ[ps, :, rows(z * 128 + di * 64, 64), :].astype(F32)
            sums.append(ZB[di, 6, sl].astype(F32) + part)
        lo, hi = sums
        first = k == 0
        put(jnp.where(first, lo[:2], hi[:2]), k, j)
        XS[j] = jnp.where(first, hi[:2], lo[:2]).astype(BF)
        swap_copy(j).start()
        for h in (0, 1):
            for cb in range(4):
                tile = sums[h][2, cb * ST : cb * ST + ST].astype(BF)
                OGD[rows(j * ST, ST), h * 512 + cb * 128 : h * 512 + cb * 128 + 128] = tile

        @pl.when(j >= 2)
        def _():
            put_swapped(j - 2)

    def mate_copy():
        return remote(MS, MR, s_m.at[0], r_m.at[0], depth=mate)

    def col_copy(dy):
        return remote(MYS.at[dy], MYR.at[dy], s_my.at[dy], r_my.at[dy], col=mod(y + dy, 4))

    def mix1():
        MS[...] = ACC[rows((1 - k) * 256, 256), :].astype(BF)
        mate_copy().start()

    def mix2():
        mate_copy().wait()
        for dy in (1, 3, 2):
            yy = mod(y + dy, 4)
            total = ACC[rows(k * 256 + yy * TD, TD), :] + MR[rows(yy * TD, TD), :].astype(F32)
            MYS[dy] = total.astype(BF)
            col_copy(dy).start()

    def mix3():
        total = ACC[rows(k * 256 + y * TD, TD), :] + MR[rows(y * TD, TD), :].astype(F32)
        for dy in (1, 3, 2):
            col_copy(dy).wait()
            total = total + MYR[dy].astype(F32)
        OM[...] = total.astype(BF)
        pltpu.make_async_copy(OM, o_mix, s_out.at[0]).start()

    def transposes():
        TT[...] = T[...].T

    stages = {"A": stage_a, "RS2": stage_rs2, "AG1": stage_ag1, "AG2": stage_ag2, "E": stage_e, "FIN": stage_fin}
    for s in range(1, 7):
        stages[f"Z{s}"] = stage_z(s)
    last_e = NC - 1 + TICK["E"] // PT

    @pl.loop(0, NC + TICK["FIN"] // PT)
    def _(i):
        for parity in range(PT):
            for name in ORDER:
                if TICK[name] % PT != parity:
                    continue
                j = i - TICK[name] // PT

                @pl.when(jnp.logical_and(j >= 0, j < NC))
                def _(name=name, j=j):
                    stages[name](j)

            if parity == 0:
                pl.when(i == 0)(transposes)
            if parity == PT - 1:
                for n, step in enumerate((mix1, mix2, mix3)):
                    pl.when(i == last_e + n)(step)

    outs = []
    outs.append(pltpu.make_async_copy(OGD, o_down, s_out.at[3]))
    outs[-1].start()
    for j in (NC - 2, NC - 1):
        put_swapped(j)
    for n, o in ((0, o_gate), (1, o_up)):
        OGB[n] = OGU[n].astype(BF)
        outs.append(pltpu.make_async_copy(OGB.at[n], o, s_out.at[1 + n]))
        outs[-1].start()
    for j in range(NC):
        swap_copy(j).wait_send()
    for a in (0, 1):
        for di in range(3):
            own_copy(a, di).wait_send()
            mate_block(a, di, own).wait_send()
        for di in (0, 1):
            relay_copy(a, di, own).wait_send()
    pltpu.make_async_copy(OM, o_mix, s_out.at[0]).wait()
    for o in outs:
        o.wait()


def written(*refs):
    ins, outs, bufs, sems = refs[:4], refs[4:8], refs[8:12], refs[12]
    there = [pltpu.make_async_copy(a, b, sems.at[0, n]) for n, (a, b) in enumerate(zip(ins, bufs))]
    back = [pltpu.make_async_copy(b, o, sems.at[1, n]) for n, (b, o) in enumerate(zip(bufs, outs))]
    for c in there:
        c.start()
    for c, w in zip(there, back):
        c.wait()
        w.start()
    for w in back:
        w.wait()


def per_device(tokens, w_gate, w_up, w_down, cotangent):
    dma = pltpu.SemaphoreType.DMA
    scratch = [
        pltpu.VMEM((TK, FW), BF),
        pltpu.VMEM((TK, FW), BF),
        pltpu.VMEM((FW, TK), BF),
        pltpu.VMEM((FW, HW), BF),
        pltpu.VMEM((FW, HW), BF),
        pltpu.VMEM((FW, 2 * CW), BF),
        pltpu.VMEM((NC, CW, FW), BF),
        pltpu.VMEM((SL, 3, TK, CW), BF),
        pltpu.VMEM((SL, 2, 3, HF, CW), BF),
        pltpu.VMEM((SL, 2, 3, OW, CW), BF),
        pltpu.VMEM((SL, 3, TK, CW), BF),
        pltpu.VMEM((PS, 3, FW, CW), BF),
        pltpu.VMEM((2, 7, ZS, 3, 64, CW), BF),
        pltpu.VMEM((TK, FW), F32),
        pltpu.VMEM((NC, 2, 64, CW), BF),
        pltpu.VMEM((NC, 2, 64, CW), BF),
        pltpu.VMEM((2, 64, HW), F32),
        pltpu.VMEM((2, 64, HW), BF),
        pltpu.VMEM((HW // 16, FW), BF),
        pltpu.VMEM((256, FW), BF),
        pltpu.VMEM((256, FW), BF),
        pltpu.VMEM((4, TD, FW), BF),
        pltpu.VMEM((4, TD, FW), BF),
        pltpu.VMEM((TD, FW), BF),
        dma((2,)), dma((2,)), dma((NC,)),
        dma((2, 3)), dma((2, 8)), dma((2, 3)), dma((2, 2)), dma((2, 2)),
        dma((2, SL)), dma((2, SL)), dma((2, SL)), dma((2, SL)),
        dma((2, SL)), dma((2, SL)), dma((2, SL)), dma((2, SL)),
        dma((2, 7, ZS)), dma((2, 7, ZS)),
        dma((NC,)), dma((NC,)),
        dma((1,)), dma((1,)), dma((4,)), dma((4,)), dma((4,)),
    ]
    anyspec = pl.BlockSpec(memory_space=pl.ANY)
    out_shape = tuple(
        jax.ShapeDtypeStruct(s, BF) for s in ((TD, FW), (FW // 16, HW), (FW // 16, HW), (HW // 16, FW))
    )
    results = pl.pallas_call(
        kernel,
        out_shape=out_shape,
        in_specs=[anyspec] * 5,
        out_specs=(anyspec,) * 4,
        scratch_shapes=scratch,
        compiler_params=pltpu.CompilerParams(
            collective_id=0, has_side_effects=True, vmem_limit_bytes=58 * 1024 * 1024
        ),
    )(tokens, w_gate, w_up, w_down, cotangent)
    return pl.pallas_call(
        written,
        out_shape=out_shape,
        in_specs=[anyspec] * 4,
        out_specs=(anyspec,) * 4,
        scratch_shapes=[pltpu.VMEM(o.shape, BF) for o in out_shape] + [dma((2, 4))],
    )(*results)


def solution(mesh):
    tok, grad = P(("col", "depth"), "row"), P(("row", "depth"), "col")
    return jax.shard_map(
        per_device,
        mesh=mesh,
        in_specs=(tok, P("row", "col"), P("row", "col"), P("col", "row"), tok),
        out_specs=(tok, grad, grad, P(("col", "depth"), "row")),
        check_vma=False,
    )
```

```python
import jax
import jax.numpy as jnp
from jax import lax
from jax.experimental import pallas as pl
from jax.experimental.pallas import tpu as pltpu
from jax.sharding import PartitionSpec as P

MESH = pl.DeviceIdType.MESH
BF, F32 = jnp.bfloat16, jnp.float32
TD, FW, HW = 64, 1024, 3584
NY, NZ = 4, 8
CW = 128
HC = HW // 2
NC = HC // CW
TK = 2 * NY * TD
OW = TK // 4
HF = OW // 2
SL, ZS, PS = 6, 6, 12
ST = CW // NZ

PT = 3
TICK = {"A": 0, "RS2": 2, "AG1": 5, "AG2": 7, "E": 9, "Z1": 12, "Z2": 14, "Z3": 17, "FIN": 20}
ORDER = ["FIN", "Z3", "Z2", "Z1", "AG2", "AG1", "RS2", "A", "E"]


def remote(src, dst, ssem, rsem, **dev):
    return pltpu.make_async_remote_copy(
        src_ref=src, dst_ref=dst, send_sem=ssem, recv_sem=rsem, device_id=dev, device_id_type=MESH
    )


def mod(a, n):
    return lax.rem(a + n, n)


def rows(start, size):
    return pl.ds(pl.multiple_of(start, size), size)


def kernel(
    tok, wg, wu, wd, cot, o_mix, o_gate, o_up, o_down,
    T, C, TT, WG, WU, WC, WD, PX, R1, R2, G, PZ, ZB, ACC, XS, XR, OGU, OGB, OGD, MS, MR, MYS, MYR, OM,
    s_in, s_w, s_wd, s_ag, r_ag, s_fw, s_rl, r_rl, s_x1, r_x1, s_x2, r_x2, s_g1, r_g1, s_g2, r_g2, s_z, r_z,
    s_xs, r_xs, s_m, r_m, s_my, r_my, s_out,
):
    r, y, d = lax.axis_index("row"), lax.axis_index("col"), lax.axis_index("depth")
    z, k = lax.div(d, 2), lax.rem(d, 2)
    right, left = mod(r + 1, 4), mod(r + 3, 4)
    opp = mod(r + 2, 4)
    zup = 2 * mod(z + 1, NZ) + k
    zdn = 2 * mod(z + NZ - 1, NZ) + k
    mate = 2 * z + (1 - k)
    own = 4 * k + y

    in_t = pltpu.make_async_copy(tok, T.at[rows(own * TD, TD), :], s_in.at[0])
    in_c = pltpu.make_async_copy(cot, C.at[rows(own * TD, TD), :], s_in.at[1])
    in_t.start()
    in_c.start()

    def start_down(j):
        for zz in range(NZ):
            src = wd.at[pl.ds(pl.multiple_of(448 * zz + 224 * k + ST * j, ST), ST), :]
            to = lax.rem(16 * (6 * k + j + 4 * (zz % 2) + zz // 2), CW)
            pltpu.make_async_copy(src, WD.at[j, rows(to, ST), :], s_wd.at[j]).start()

    def wide_copy(n, q):
        at = pl.ds(q * 256, 256)
        return pltpu.make_async_copy((wg, wu)[n].at[at, :], (WG, WU)[n].at[at, :], s_w.at[n])

    barrier = pltpu.get_barrier_semaphore()
    for other in (right, left):
        pl.semaphore_signal(barrier, inc=1, device_id={"row": other}, device_id_type=MESH)
    for dy in range(1, 4):
        pl.semaphore_signal(barrier, inc=1, device_id={"col": mod(y + dy, 4)}, device_id_type=MESH)
    for other in (zup, zdn, mate):
        pl.semaphore_signal(barrier, inc=1, device_id={"depth": other}, device_id_type=MESH)

    for n in (0, 1):
        for q in range(4):
            wide_copy(n, q).start()
    pl.loop(0, NC)(start_down)
    ACC[...] = jnp.zeros_like(ACC)
    pl.semaphore_wait(barrier, 8)

    def lane_block(kk, j, zz):
        return rows(lax.div(448 * zz + 224 * kk + ST * j, CW) * CW, CW)

    def strip_at(j):
        lane = lax.broadcasted_iota(jnp.int32, (128, CW), 1)
        u = lax.rem(lax.div(lane, ST) + 16 - lax.rem(6 * k + j, 8), 8)
        return 2 * lax.rem(u, 4) + lax.div(u, 4)

    def chunk_weights(j):
        which = strip_at(j)
        for n, buf in enumerate((WG, WU)):
            for q in range(8):
                at = pl.ds(q * 128, 128)
                got = buf[at, lane_block(k, j, 0)]
                for zz in range(1, NZ):
                    part = buf[at, lane_block(k, j, zz)]
                    if zz // 2:
                        part = pltpu.roll(part, ST * (zz // 2), 1)
                    got = jnp.where(which == zz, part, got)
                WC[lax.rem(j, 2), at, n * CW : (n + 1) * CW] = got

    def block_of(a, b):
        return (T, C)[a].at[rows(b * TD, TD), :]

    yto = (mod(y + 1, 4), mod(y + 3, 4))
    yop = 4 * k + mod(y + 2, 4)

    def own_copy(a, di):
        dev = {"depth": mate} if di == 2 else {"col": yto[di]}
        return remote(block_of(a, own), block_of(a, own), s_ag.at[a, di], r_ag.at[a, own], **dev)

    def relay_copy(a, di, b):
        at = (T, C)[a].at[rows(b * TD + di * (TD // 2), TD // 2), :]
        return remote(at, at, s_rl.at[a, di], r_rl.at[a, di], col=yto[di])

    def mate_block(a, n, b):
        return remote(block_of(a, b), block_of(a, b), s_fw.at[a, n], r_ag.at[a, b], depth=mate)

    for a, mine in ((0, in_t), (1, in_c)):
        mine.wait()
        for di in range(3):
            own_copy(a, di).start()
    for a in (0, 1):
        for di in (0, 1):
            b = 4 * k + yto[1 - di]
            mate_block(a, di, b).wait_recv()
            relay_copy(a, di, b).start()
            mate_block(a, di, b).start()
    for a in (0, 1):
        for di in (0, 1):
            relay_copy(a, di, yop).wait_recv()
        mate_block(a, 2, yop).start()
    for n, (w, buf) in enumerate(((wg, WG), (wu, WU))):
        pltpu.make_async_copy(w, buf, s_w.at[n]).wait()
    chunk_weights(0)
    for a in (0, 1):
        for yy in range(4):
            mate_block(a, 0, 4 * (1 - k) + yy).wait_recv()

    def xto(di):
        return {"row": (right, left)[di]}

    def x1_copy(j, di):
        sl = lax.rem(j, SL)
        src = PX.at[sl, :, rows(opp * OW + di * HF, HF), :]
        return remote(src, R1.at[sl, di], s_x1.at[di, sl], r_x1.at[di, sl], **xto(di))

    def x2_copy(j, di):
        sl = lax.rem(j, SL)
        src = PX.at[sl, :, rows((right, left)[di] * OW, OW), :]
        return remote(src, R2.at[sl, di], s_x2.at[di, sl], r_x2.at[di, sl], **xto(di))

    def g1_copy(j, di, owner):
        sl = lax.rem(j, SL)
        at = G.at[sl, :, rows(owner * OW, OW), :]
        return remote(at, at, s_g1.at[di, sl], r_g1.at[di, sl], **xto(di))

    def g2_copy(j, di, owner):
        sl = lax.rem(j, SL)
        at = G.at[sl, :, rows(owner * OW + di * HF, HF), :]
        return remote(at, at, s_g2.at[di, sl], r_g2.at[di, sl], **xto(di))

    def zblock(di, s):
        return (mod(z + 4 - s, NZ) if di == 0 else mod(z + 4 + s, NZ)) * 128

    def z_copy(j, di, s):
        sl = lax.rem(j, ZS)
        if s == 0:
            half = pl.ds(di * 64, 64)
            src = PZ.at[lax.rem(j, PS), :, rows(zblock(di, 0) + di * 64, 64), :]
            dst = ZB.at[di, 0, sl, :, half, :]
        else:
            src, dst = ZB.at[di, s - 1, sl], ZB.at[di, s, sl]
        return remote(src, dst, s_z.at[di, s, sl], r_z.at[di, s, sl], depth=(zup, zdn)[di])

    def stage_a(j):
        sl = lax.rem(j, SL)
        pltpu.make_async_copy(wd.at[pl.ds(0, CW), :], WD.at[j], s_wd.at[j]).wait()
        for m in range(2):
            at = pl.ds(m * 256, 256)
            gu = jnp.dot(T[at, :], WC[lax.rem(j, 2)], preferred_element_type=F32)
            h = lax.dot_general(C[at, :], WD[j], (((1,), (1,)), ((), ())), preferred_element_type=F32)
            PX[sl, 0, at, :] = gu[:, :CW].astype(BF)
            PX[sl, 1, at, :] = gu[:, CW:].astype(BF)
            PX[sl, 2, at, :] = h.astype(BF)
        for di in (0, 1):
            x1_copy(j, di).start()

    def stage_rs2(j):
        sl = lax.rem(j, SL)
        for di in (0, 1):
            x1_copy(j, di).wait_recv()
            at = rows((right, left)[di] * OW + di * HF, HF)
            PX[sl, :, at, :] = (PX[sl, :, at, :].astype(F32) + R1[sl, di].astype(F32)).astype(BF)
            x2_copy(j, di).start()

    def stage_ag1(j):
        sl = lax.rem(j, SL)
        for di in (0, 1):
            x1_copy(j, di).wait_send()
        for di in (0, 1):
            x2_copy(j, di).wait_recv()
        at = rows(r * OW, OW)
        total = PX[sl, :, at, :].astype(F32) + R2[sl, 0].astype(F32) + R2[sl, 1].astype(F32)
        gate, up, hg = total[0], total[1], total[2]
        sig = jax.nn.sigmoid(gate)
        G[sl, 0, at, :] = (gate * sig * up).astype(BF)
        G[sl, 1, at, :] = (hg * up * sig * (1.0 + gate * (1.0 - sig))).astype(BF)
        G[sl, 2, at, :] = (hg * gate * sig).astype(BF)
        for di in (0, 1):
            g1_copy(j, di, r).start()

    def stage_ag2(j):
        for di in (0, 1):
            frm = (left, right)[di]
            g1_copy(j, di, frm).wait_recv()
            g2_copy(j, di, frm).start()

    def stage_e(j):
        sl, ps = lax.rem(j, SL), lax.rem(j, PS)
        for di in (0, 1):
            x2_copy(j, di).wait_send()
            g1_copy(j, di, r).wait_send()
        for di in (0, 1):
            g2_copy(j, di, opp).wait_recv()
        hid = G[sl, 0]
        dgu = jnp.concatenate([G[sl, 1], G[sl, 2]], axis=1)
        for m in range(4):
            at = pl.ds(m * 256, 256)
            gu = jnp.dot(TT[at, :], dgu, preferred_element_type=F32)
            PZ[ps, 0, at, :] = gu[:, :CW].astype(BF)
            PZ[ps, 1, at, :] = gu[:, CW:].astype(BF)
        hid_t = hid.T
        for h in range(2):
            down = jnp.dot(hid_t, C[:, h * 512 : h * 512 + 512], preferred_element_type=F32).astype(BF)
            for ub in range(8):
                u = lax.rem(ub + 16 - lax.rem(6 * k + j, 8), 8)
                top = (2 * lax.rem(u, 4) + lax.div(u, 4)) * 128 + h * 64
                for cb in range(4):
                    tile = down[ub * ST : ub * ST + ST, cb * 128 : cb * 128 + 128]
                    PZ[ps, 2, pl.ds(pl.multiple_of(top + cb * ST, ST), ST), :] = tile
        for di in (0, 1):
            z_copy(j, di, 0).start()
        for m in range(4):
            at = pl.ds(m * 128, 128)
            ACC[at, :] += jnp.dot(G[sl, 0, at, :], WD[j], preferred_element_type=F32)

    def stage_z(s):
        def run(j):
            sl, ps = lax.rem(j, ZS), lax.rem(j, PS)
            if s == 1:
                for di in (0, 1):
                    g2_copy(j, di, (left, right)[di]).wait_send()
            else:
                for di in (0, 1):
                    z_copy(j, di, s - 2).wait_send()
            for di in (0, 1):
                z_copy(j, di, s - 1).wait_recv()
                for h in (0, 1):
                    at = pl.ds(h * 64, 64)
                    part = PZ[ps, :, rows(zblock(di, s) + h * 64, 64), :]
                    if s > 1 or h == di:
                        part = (part.astype(F32) + ZB[di, s - 1, sl, :, at, :].astype(F32)).astype(BF)
                    ZB[di, s - 1, sl, :, at, :] = part
                z_copy(j, di, s).start()

        return run

    def swap_copy(j):
        return remote(XS.at[j], XR.at[j], s_xs.at[j], r_xs.at[j], depth=mate)

    def put(value, kk, j):
        lane = lax.div(lax.broadcasted_iota(jnp.int32, (2, 64, CW), 2), ST)
        for g in range(4):
            turned = pltpu.roll(value, CW - ST * g, 2) if g else value
            for zz in (2 * g, 2 * g + 1):
                at = lane_block(kk, j, zz)
                here = lane == lax.rem(4 * zz + 6 * kk + j, 8)
                OGU[:, :, at] = jnp.where(here, turned, OGU[:, :, at])

    def put_swapped(j):
        swap_copy(j).wait_recv()
        put(XR[j].astype(F32), 1 - k, j)

    def stage_fin(j):
        sl, ps = lax.rem(j, ZS), lax.rem(j, PS)
        sums = []
        for di in (0, 1):
            for s in (2, 3):
                z_copy(j, di, s).wait_send()
        for di in (0, 1):
            z_copy(j, di, 3).wait_recv()
        for h in (0, 1):
            at = pl.ds(h * 64, 64)
            part = PZ[ps, :, rows(z * 128 + h * 64, 64), :].astype(F32)
            sums.append(part + ZB[0, 3, sl, :, at, :].astype(F32) + ZB[1, 3, sl, :, at, :].astype(F32))
        lo, hi = sums
        first = k == 0
        put(jnp.where(first, lo[:2], hi[:2]), k, j)
        XS[j] = jnp.where(first, hi[:2], lo[:2]).astype(BF)
        swap_copy(j).start()
        for h in (0, 1):
            for cb in range(4):
                tile = sums[h][2, cb * ST : cb * ST + ST].astype(BF)
                OGD[rows(j * ST, ST), h * 512 + cb * 128 : h * 512 + cb * 128 + 128] = tile

        @pl.when(j >= 2)
        def _():
            put_swapped(j - 2)

    def mate_copy():
        return remote(MS, MR, s_m.at[0], r_m.at[0], depth=mate)

    def col_copy(dy):
        return remote(MYS.at[dy], MYR.at[dy], s_my.at[dy], r_my.at[dy], col=mod(y + dy, 4))

    def mix1():
        MS[...] = ACC[rows((1 - k) * 256, 256), :].astype(BF)
        mate_copy().start()

    def mix2():
        mate_copy().wait()
        for dy in (1, 3, 2):
            yy = mod(y + dy, 4)
            total = ACC[rows(k * 256 + yy * TD, TD), :] + MR[rows(yy * TD, TD), :].astype(F32)
            MYS[dy] = total.astype(BF)
            col_copy(dy).start()

    def mix3():
        total = ACC[rows(k * 256 + y * TD, TD), :] + MR[rows(y * TD, TD), :].astype(F32)
        for dy in (1, 3, 2):
            col_copy(dy).wait()
            total = total + MYR[dy].astype(F32)
        OM[...] = total.astype(BF)
        pltpu.make_async_copy(OM, o_mix, s_out.at[0]).start()

    def transposes():
        TT[...] = T[...].T

    stages = {"A": stage_a, "RS2": stage_rs2, "AG1": stage_ag1, "AG2": stage_ag2, "E": stage_e, "FIN": stage_fin}
    for s in range(1, 4):
        stages[f"Z{s}"] = stage_z(s)
    last_e = NC - 1 + TICK["E"] // PT

    @pl.loop(0, NC + TICK["FIN"] // PT)
    def _(i):
        for parity in range(PT):
            for name in ORDER:
                if TICK[name] % PT != parity:
                    continue
                j = i - TICK[name] // PT

                @pl.when(jnp.logical_and(j >= 0, j < NC))
                def _(name=name, j=j):
                    stages[name](j)

            if parity == 0:
                pl.when(i == 0)(transposes)
            if parity == PT - 1:
                pl.when(i < NC - 1)(lambda: chunk_weights(i + 1))
                for n, step in enumerate((mix1, mix2, mix3)):
                    pl.when(i == last_e + n)(step)

    outs = []
    outs.append(pltpu.make_async_copy(OGD, o_down, s_out.at[3]))
    outs[-1].start()
    for j in (NC - 2, NC - 1):
        put_swapped(j)
    for n, o in ((0, o_gate), (1, o_up)):
        OGB[n] = OGU[n].astype(BF)
        outs.append(pltpu.make_async_copy(OGB.at[n], o, s_out.at[1 + n]))
        outs[-1].start()
    for j in range(NC):
        swap_copy(j).wait_send()
    for a in (0, 1):
        for di in range(3):
            own_copy(a, di).wait_send()
            mate_block(a, di, own).wait_send()
        for di in (0, 1):
            relay_copy(a, di, own).wait_send()
    pltpu.make_async_copy(OM, o_mix, s_out.at[0]).wait()
    for o in outs:
        o.wait()


def written(*refs):
    ins, outs, bufs, sems = refs[:4], refs[4:8], refs[8:12], refs[12]
    there = [pltpu.make_async_copy(a, b, sems.at[0, n]) for n, (a, b) in enumerate(zip(ins, bufs))]
    back = [pltpu.make_async_copy(b, o, sems.at[1, n]) for n, (b, o) in enumerate(zip(bufs, outs))]
    for c in there:
        c.start()
    for c, w in zip(there, back):
        c.wait()
        w.start()
    for w in back:
        w.wait()


def per_device(tokens, w_gate, w_up, w_down, cotangent):
    dma = pltpu.SemaphoreType.DMA
    scratch = [
        pltpu.VMEM((TK, FW), BF),
        pltpu.VMEM((TK, FW), BF),
        pltpu.VMEM((FW, TK), BF),
        pltpu.VMEM((FW, HW), BF),
        pltpu.VMEM((FW, HW), BF),
        pltpu.VMEM((2, FW, 2 * CW), BF),
        pltpu.VMEM((NC, CW, FW), BF),
        pltpu.VMEM((SL, 3, TK, CW), BF),
        pltpu.VMEM((SL, 2, 3, HF, CW), BF),
        pltpu.VMEM((SL, 2, 3, OW, CW), BF),
        pltpu.VMEM((SL, 3, TK, CW), BF),
        pltpu.VMEM((PS, 3, FW, CW), BF),
        pltpu.VMEM((2, 4, ZS, 3, 128, CW), BF),
        pltpu.VMEM((TK, FW), F32),
        pltpu.VMEM((NC, 2, 64, CW), BF),
        pltpu.VMEM((NC, 2, 64, CW), BF),
        pltpu.VMEM((2, 64, HW), F32),
        pltpu.VMEM((2, 64, HW), BF),
        pltpu.VMEM((HW // 16, FW), BF),
        pltpu.VMEM((256, FW), BF),
        pltpu.VMEM((256, FW), BF),
        pltpu.VMEM((4, TD, FW), BF),
        pltpu.VMEM((4, TD, FW), BF),
        pltpu.VMEM((TD, FW), BF),
        dma((2,)), dma((2,)), dma((NC,)),
        dma((2, 3)), dma((2, 8)), dma((2, 3)), dma((2, 2)), dma((2, 2)),
        dma((2, SL)), dma((2, SL)), dma((2, SL)), dma((2, SL)),
        dma((2, SL)), dma((2, SL)), dma((2, SL)), dma((2, SL)),
        dma((2, 4, ZS)), dma((2, 4, ZS)),
        dma((NC,)), dma((NC,)),
        dma((1,)), dma((1,)), dma((4,)), dma((4,)), dma((4,)),
    ]
    anyspec = pl.BlockSpec(memory_space=pl.ANY)
    out_shape = tuple(
        jax.ShapeDtypeStruct(s, BF) for s in ((TD, FW), (FW // 16, HW), (FW // 16, HW), (HW // 16, FW))
    )
    results = pl.pallas_call(
        kernel,
        out_shape=out_shape,
        in_specs=[anyspec] * 5,
        out_specs=(anyspec,) * 4,
        scratch_shapes=scratch,
        compiler_params=pltpu.CompilerParams(
            collective_id=0, has_side_effects=True, vmem_limit_bytes=58 * 1024 * 1024
        ),
    )(tokens, w_gate, w_up, w_down, cotangent)
    return pl.pallas_call(
        written,
        out_shape=out_shape,
        in_specs=[anyspec] * 4,
        out_specs=(anyspec,) * 4,
        scratch_shapes=[pltpu.VMEM(o.shape, BF) for o in out_shape] + [dma((2, 4))],
    )(*results)


def solution(mesh):
    tok, grad = P(("col", "depth"), "row"), P(("row", "depth"), "col")
    return jax.shard_map(
        per_device,
        mesh=mesh,
        in_specs=(tok, P("row", "col"), P("row", "col"), P("col", "row"), tok),
        out_specs=(tok, grad, grad, P(("col", "depth"), "row")),
        check_vma=False,
    )
```

```python
import jax
import jax.numpy as jnp
from jax import lax
from jax.experimental import pallas as pl
from jax.experimental.pallas import tpu as pltpu
from jax.sharding import PartitionSpec as P

MESH = pl.DeviceIdType.MESH
BF, F32 = jnp.bfloat16, jnp.float32
TD, FW, HW = 64, 1024, 3584
NY, NZ = 4, 8
CW = 128
HC = HW // 2
NC = HC // CW
TK = 2 * NY * TD
OW = TK // 4
HF = OW // 2
SL, ZS, PS = 6, 6, 12
ST = CW // NZ

PT = 3
TICK = {"A": 0, "RS2": 2, "AG1": 5, "AG2": 8, "E": 10, "Z1": 13, "Z2": 16, "Z3": 19, "FIN": 22}
ORDER = ["FIN", "Z3", "Z2", "Z1", "AG2", "AG1", "RS2", "A", "E"]


def remote(src, dst, ssem, rsem, **dev):
    return pltpu.make_async_remote_copy(
        src_ref=src, dst_ref=dst, send_sem=ssem, recv_sem=rsem, device_id=dev, device_id_type=MESH
    )


def mod(a, n):
    return lax.rem(a + n, n)


def rows(start, size):
    return pl.ds(pl.multiple_of(start, size), size)


def kernel(
    tok, wg, wu, wd, cot, o_mix, o_gate, o_up, o_down,
    T, C, TT, WG, WU, WC, WD, PX, R1, R2, G, PZ, ZB, ACC, XS, XR, OGU, OGB, OGD, MS, MR, MYS, MYR, OM,
    s_in, s_w, s_wd, s_ag, r_ag, s_fw, s_rl, r_rl, s_x1, r_x1, s_x2, r_x2, s_g1, r_g1, s_g2, r_g2, s_z, r_z,
    s_xs, r_xs, s_m, r_m, s_my, r_my, s_out,
):
    r, y, d = lax.axis_index("row"), lax.axis_index("col"), lax.axis_index("depth")
    z, k = lax.div(d, 2), lax.rem(d, 2)
    right, left = mod(r + 1, 4), mod(r + 3, 4)
    opp = mod(r + 2, 4)
    zup = 2 * mod(z + 1, NZ) + k
    zdn = 2 * mod(z + NZ - 1, NZ) + k
    mate = 2 * z + (1 - k)
    own = 4 * k + y

    in_t = pltpu.make_async_copy(tok, T.at[rows(own * TD, TD), :], s_in.at[0])
    in_c = pltpu.make_async_copy(cot, C.at[rows(own * TD, TD), :], s_in.at[1])
    in_t.start()
    in_c.start()

    def start_down(j):
        for zz in range(NZ):
            src = wd.at[pl.ds(pl.multiple_of(448 * zz + 224 * k + ST * j, ST), ST), :]
            to = lax.rem(16 * (6 * k + j + 4 * (zz % 2) + zz // 2), CW)
            pltpu.make_async_copy(src, WD.at[j, rows(to, ST), :], s_wd.at[j]).start()

    def wide_copy(n, q):
        at = pl.ds(q * 256, 256)
        return pltpu.make_async_copy((wg, wu)[n].at[at, :], (WG, WU)[n].at[at, :], s_w.at[n])

    barrier = pltpu.get_barrier_semaphore()
    for other in (right, left):
        pl.semaphore_signal(barrier, inc=1, device_id={"row": other}, device_id_type=MESH)
    for dy in range(1, 4):
        pl.semaphore_signal(barrier, inc=1, device_id={"col": mod(y + dy, 4)}, device_id_type=MESH)
    for other in (zup, zdn, mate):
        pl.semaphore_signal(barrier, inc=1, device_id={"depth": other}, device_id_type=MESH)

    for n in (0, 1):
        for q in range(4):
            wide_copy(n, q).start()
    pl.loop(0, NC)(start_down)
    ACC[...] = jnp.zeros_like(ACC)
    pl.semaphore_wait(barrier, 8)

    def lane_block(kk, j, zz):
        return rows(lax.div(448 * zz + 224 * kk + ST * j, CW) * CW, CW)

    def strip_at(j):
        lane = lax.broadcasted_iota(jnp.int32, (128, CW), 1)
        u = lax.rem(lax.div(lane, ST) + 16 - lax.rem(6 * k + j, 8), 8)
        return 2 * lax.rem(u, 4) + lax.div(u, 4)

    def chunk_weights(j):
        which = strip_at(j)
        for n, buf in enumerate((WG, WU)):
            for q in range(8):
                at = pl.ds(q * 128, 128)
                got = buf[at, lane_block(k, j, 0)]
                for zz in range(1, NZ):
                    part = buf[at, lane_block(k, j, zz)]
                    if zz // 2:
                        part = pltpu.roll(part, ST * (zz // 2), 1)
                    got = jnp.where(which == zz, part, got)
                WC[lax.rem(j, 2), at, n * CW : (n + 1) * CW] = got

    def block_of(a, b):
        return (T, C)[a].at[rows(b * TD, TD), :]

    yto = (mod(y + 1, 4), mod(y + 3, 4))
    yop = 4 * k + mod(y + 2, 4)

    def own_copy(a, di):
        dev = {"depth": mate} if di == 2 else {"col": yto[di]}
        return remote(block_of(a, own), block_of(a, own), s_ag.at[a, di], r_ag.at[a, own], **dev)

    def relay_copy(a, di, b):
        at = (T, C)[a].at[rows(b * TD + di * (TD // 2), TD // 2), :]
        return remote(at, at, s_rl.at[a, di], r_rl.at[a, di], col=yto[di])

    def mate_block(a, n, b):
        return remote(block_of(a, b), block_of(a, b), s_fw.at[a, n], r_ag.at[a, b], depth=mate)

    for a, mine in ((0, in_t), (1, in_c)):
        mine.wait()
        for di in range(3):
            own_copy(a, di).start()
    for a in (0, 1):
        for di in (0, 1):
            b = 4 * k + yto[1 - di]
            mate_block(a, di, b).wait_recv()
            relay_copy(a, di, b).start()
            mate_block(a, di, b).start()
    for a in (0, 1):
        for di in (0, 1):
            relay_copy(a, di, yop).wait_recv()
        mate_block(a, 2, yop).start()
    for n, (w, buf) in enumerate(((wg, WG), (wu, WU))):
        pltpu.make_async_copy(w, buf, s_w.at[n]).wait()
    chunk_weights(0)
    for a in (0, 1):
        for yy in range(4):
            mate_block(a, 0, 4 * (1 - k) + yy).wait_recv()

    def xto(di):
        return {"row": (right, left)[di]}

    def x1_copy(j, di):
        sl = lax.rem(j, SL)
        src = PX.at[sl, :, rows(opp * OW + di * HF, HF), :]
        return remote(src, R1.at[sl, di], s_x1.at[di, sl], r_x1.at[di, sl], **xto(di))

    def x2_copy(j, di):
        sl = lax.rem(j, SL)
        src = PX.at[sl, :, rows((right, left)[di] * OW, OW), :]
        return remote(src, R2.at[sl, di], s_x2.at[di, sl], r_x2.at[di, sl], **xto(di))

    def g1_copy(j, di, owner):
        sl = lax.rem(j, SL)
        at = G.at[sl, :, rows(owner * OW, OW), :]
        return remote(at, at, s_g1.at[di, sl], r_g1.at[di, sl], **xto(di))

    def g2_copy(j, di, owner):
        sl = lax.rem(j, SL)
        at = G.at[sl, :, rows(owner * OW + di * HF, HF), :]
        return remote(at, at, s_g2.at[di, sl], r_g2.at[di, sl], **xto(di))

    def zblock(di, s):
        return (mod(z + 4 - s, NZ) if di == 0 else mod(z + 4 + s, NZ)) * 128

    def z_copy(j, di, s):
        sl = lax.rem(j, ZS)
        if s == 0:
            half = pl.ds(di * 64, 64)
            src = PZ.at[lax.rem(j, PS), :, rows(zblock(di, 0) + di * 64, 64), :]
            dst = ZB.at[di, 0, sl, :, half, :]
        else:
            src, dst = ZB.at[di, s - 1, sl], ZB.at[di, s, sl]
        return remote(src, dst, s_z.at[di, s, sl], r_z.at[di, s, sl], depth=(zup, zdn)[di])

    def stage_a(j):
        sl = lax.rem(j, SL)
        pltpu.make_async_copy(wd.at[pl.ds(0, CW), :], WD.at[j], s_wd.at[j]).wait()
        for m in range(2):
            at = pl.ds(m * 256, 256)
            gu = jnp.dot(T[at, :], WC[lax.rem(j, 2)], preferred_element_type=F32)
            h = lax.dot_general(C[at, :], WD[j], (((1,), (1,)), ((), ())), preferred_element_type=F32)
            PX[sl, 0, at, :] = gu[:, :CW].astype(BF)
            PX[sl, 1, at, :] = gu[:, CW:].astype(BF)
            PX[sl, 2, at, :] = h.astype(BF)
        for di in (0, 1):
            x1_copy(j, di).start()

    def stage_rs2(j):
        sl = lax.rem(j, SL)
        for di in (0, 1):
            x1_copy(j, di).wait_recv()
            at = rows((right, left)[di] * OW + di * HF, HF)
            PX[sl, :, at, :] = (PX[sl, :, at, :].astype(F32) + R1[sl, di].astype(F32)).astype(BF)
            x2_copy(j, di).start()

    def stage_ag1(j):
        sl = lax.rem(j, SL)
        for di in (0, 1):
            x1_copy(j, di).wait_send()
        for di in (0, 1):
            x2_copy(j, di).wait_recv()
        at = rows(r * OW, OW)
        total = PX[sl, :, at, :].astype(F32) + R2[sl, 0].astype(F32) + R2[sl, 1].astype(F32)
        gate, up, hg = total[0], total[1], total[2]
        sig = jax.nn.sigmoid(gate)
        G[sl, 0, at, :] = (gate * sig * up).astype(BF)
        G[sl, 1, at, :] = (hg * up * sig * (1.0 + gate * (1.0 - sig))).astype(BF)
        G[sl, 2, at, :] = (hg * gate * sig).astype(BF)
        for di in (0, 1):
            g1_copy(j, di, r).start()

    def stage_ag2(j):
        for di in (0, 1):
            frm = (left, right)[di]
            g1_copy(j, di, frm).wait_recv()
            g2_copy(j, di, frm).start()

    def stage_e(j):
        sl, ps = lax.rem(j, SL), lax.rem(j, PS)
        for di in (0, 1):
            x2_copy(j, di).wait_send()
            g1_copy(j, di, r).wait_send()
        for di in (0, 1):
            g2_copy(j, di, opp).wait_recv()
        hid = G[sl, 0]
        dgu = jnp.concatenate([G[sl, 1], G[sl, 2]], axis=1)
        for m in range(4):
            at = pl.ds(m * 256, 256)
            gu = jnp.dot(TT[at, :], dgu, preferred_element_type=F32)
            PZ[ps, 0, at, :] = gu[:, :CW].astype(BF)
            PZ[ps, 1, at, :] = gu[:, CW:].astype(BF)
        hid_t = hid.T
        for h in range(2):
            down = jnp.dot(hid_t, C[:, h * 512 : h * 512 + 512], preferred_element_type=F32).astype(BF)
            for ub in range(8):
                u = lax.rem(ub + 16 - lax.rem(6 * k + j, 8), 8)
                top = (2 * lax.rem(u, 4) + lax.div(u, 4)) * 128 + h * 64
                for cb in range(4):
                    tile = down[ub * ST : ub * ST + ST, cb * 128 : cb * 128 + 128]
                    PZ[ps, 2, pl.ds(pl.multiple_of(top + cb * ST, ST), ST), :] = tile
        for di in (0, 1):
            z_copy(j, di, 0).start()
        for m in range(4):
            at = pl.ds(m * 128, 128)
            ACC[at, :] += jnp.dot(G[sl, 0, at, :], WD[j], preferred_element_type=F32)

    def stage_z(s):
        def run(j):
            sl, ps = lax.rem(j, ZS), lax.rem(j, PS)
            if s == 1:
                for di in (0, 1):
                    g2_copy(j, di, (left, right)[di]).wait_send()
            else:
                for di in (0, 1):
                    z_copy(j, di, s - 2).wait_send()
            for di in (0, 1):
                z_copy(j, di, s - 1).wait_recv()
                for h in (0, 1):
                    at = pl.ds(h * 64, 64)
                    part = PZ[ps, :, rows(zblock(di, s) + h * 64, 64), :]
                    if s > 1 or h == di:
                        part = (part.astype(F32) + ZB[di, s - 1, sl, :, at, :].astype(F32)).astype(BF)
                    ZB[di, s - 1, sl, :, at, :] = part
                z_copy(j, di, s).start()

        return run

    def swap_copy(j):
        return remote(XS.at[j], XR.at[j], s_xs.at[j], r_xs.at[j], depth=mate)

    def put(value, kk, j):
        lane = lax.div(lax.broadcasted_iota(jnp.int32, (2, 64, CW), 2), ST)
        for g in range(4):
            turned = pltpu.roll(value, CW - ST * g, 2) if g else value
            for zz in (2 * g, 2 * g + 1):
                at = lane_block(kk, j, zz)
                here = lane == lax.rem(4 * zz + 6 * kk + j, 8)
                OGU[:, :, at] = jnp.where(here, turned, OGU[:, :, at])

    def put_swapped(j):
        swap_copy(j).wait_recv()
        put(XR[j].astype(F32), 1 - k, j)

    def stage_fin(j):
        sl, ps = lax.rem(j, ZS), lax.rem(j, PS)
        sums = []
        for di in (0, 1):
            for s in (2, 3):
                z_copy(j, di, s).wait_send()
        for di in (0, 1):
            z_copy(j, di, 3).wait_recv()
        for h in (0, 1):
            at = pl.ds(h * 64, 64)
            part = PZ[ps, :, rows(z * 128 + h * 64, 64), :].astype(F32)
            sums.append(part + ZB[0, 3, sl, :, at, :].astype(F32) + ZB[1, 3, sl, :, at, :].astype(F32))
        lo, hi = sums
        first = k == 0
        put(jnp.where(first, lo[:2], hi[:2]), k, j)
        XS[j] = jnp.where(first, hi[:2], lo[:2]).astype(BF)
        swap_copy(j).start()
        for h in (0, 1):
            for cb in range(4):
                tile = sums[h][2, cb * ST : cb * ST + ST].astype(BF)
                OGD[rows(j * ST, ST), h * 512 + cb * 128 : h * 512 + cb * 128 + 128] = tile

        @pl.when(j >= 2)
        def _():
            put_swapped(j - 2)

    def mate_copy():
        return remote(MS, MR, s_m.at[0], r_m.at[0], depth=mate)

    def col_copy(dy):
        return remote(MYS.at[dy], MYR.at[dy], s_my.at[dy], r_my.at[dy], col=mod(y + dy, 4))

    def mix1():
        MS[...] = ACC[rows((1 - k) * 256, 256), :].astype(BF)
        mate_copy().start()

    def mix2():
        mate_copy().wait()
        for dy in (1, 3, 2):
            yy = mod(y + dy, 4)
            total = ACC[rows(k * 256 + yy * TD, TD), :] + MR[rows(yy * TD, TD), :].astype(F32)
            MYS[dy] = total.astype(BF)
            col_copy(dy).start()

    def mix3():
        total = ACC[rows(k * 256 + y * TD, TD), :] + MR[rows(y * TD, TD), :].astype(F32)
        for dy in (1, 3, 2):
            col_copy(dy).wait()
            total = total + MYR[dy].astype(F32)
        OM[...] = total.astype(BF)
        pltpu.make_async_copy(OM, o_mix, s_out.at[0]).start()

    def transposes():
        TT[...] = T[...].T

    stages = {"A": stage_a, "RS2": stage_rs2, "AG1": stage_ag1, "AG2": stage_ag2, "E": stage_e, "FIN": stage_fin}
    for s in range(1, 4):
        stages[f"Z{s}"] = stage_z(s)
    last_e = NC - 1 + TICK["E"] // PT

    @pl.loop(0, NC + TICK["FIN"] // PT)
    def _(i):
        for parity in range(PT):
            for name in ORDER:
                if TICK[name] % PT != parity:
                    continue
                j = i - TICK[name] // PT

                @pl.when(jnp.logical_and(j >= 0, j < NC))
                def _(name=name, j=j):
                    stages[name](j)

            if parity == 0:
                pl.when(i == 0)(transposes)
            if parity == PT - 1:
                pl.when(i < NC - 1)(lambda: chunk_weights(i + 1))
                for n, step in enumerate((mix1, mix2, mix3)):
                    pl.when(i == last_e + n)(step)

    outs = []
    outs.append(pltpu.make_async_copy(OGD, o_down, s_out.at[3]))
    outs[-1].start()
    for j in (NC - 2, NC - 1):
        put_swapped(j)
    for n, o in ((0, o_gate), (1, o_up)):
        OGB[n] = OGU[n].astype(BF)
        outs.append(pltpu.make_async_copy(OGB.at[n], o, s_out.at[1 + n]))
        outs[-1].start()
    for j in range(NC):
        swap_copy(j).wait_send()
    for a in (0, 1):
        for di in range(3):
            own_copy(a, di).wait_send()
            mate_block(a, di, own).wait_send()
        for di in (0, 1):
            relay_copy(a, di, own).wait_send()
    pltpu.make_async_copy(OM, o_mix, s_out.at[0]).wait()
    for o in outs:
        o.wait()


def written(*refs):
    ins, outs, bufs, sems = refs[:4], refs[4:8], refs[8:12], refs[12]
    there = [pltpu.make_async_copy(a, b, sems.at[0, n]) for n, (a, b) in enumerate(zip(ins, bufs))]
    back = [pltpu.make_async_copy(b, o, sems.at[1, n]) for n, (b, o) in enumerate(zip(bufs, outs))]
    for c in there:
        c.start()
    for c, w in zip(there, back):
        c.wait()
        w.start()
    for w in back:
        w.wait()


def per_device(tokens, w_gate, w_up, w_down, cotangent):
    dma = pltpu.SemaphoreType.DMA
    scratch = [
        pltpu.VMEM((TK, FW), BF),
        pltpu.VMEM((TK, FW), BF),
        pltpu.VMEM((FW, TK), BF),
        pltpu.VMEM((FW, HW), BF),
        pltpu.VMEM((FW, HW), BF),
        pltpu.VMEM((2, FW, 2 * CW), BF),
        pltpu.VMEM((NC, CW, FW), BF),
        pltpu.VMEM((SL, 3, TK, CW), BF),
        pltpu.VMEM((SL, 2, 3, HF, CW), BF),
        pltpu.VMEM((SL, 2, 3, OW, CW), BF),
        pltpu.VMEM((SL, 3, TK, CW), BF),
        pltpu.VMEM((PS, 3, FW, CW), BF),
        pltpu.VMEM((2, 4, ZS, 3, 128, CW), BF),
        pltpu.VMEM((TK, FW), F32),
        pltpu.VMEM((NC, 2, 64, CW), BF),
        pltpu.VMEM((NC, 2, 64, CW), BF),
        pltpu.VMEM((2, 64, HW), F32),
        pltpu.VMEM((2, 64, HW), BF),
        pltpu.VMEM((HW // 16, FW), BF),
        pltpu.VMEM((256, FW), BF),
        pltpu.VMEM((256, FW), BF),
        pltpu.VMEM((4, TD, FW), BF),
        pltpu.VMEM((4, TD, FW), BF),
        pltpu.VMEM((TD, FW), BF),
        dma((2,)), dma((2,)), dma((NC,)),
        dma((2, 3)), dma((2, 8)), dma((2, 3)), dma((2, 2)), dma((2, 2)),
        dma((2, SL)), dma((2, SL)), dma((2, SL)), dma((2, SL)),
        dma((2, SL)), dma((2, SL)), dma((2, SL)), dma((2, SL)),
        dma((2, 4, ZS)), dma((2, 4, ZS)),
        dma((NC,)), dma((NC,)),
        dma((1,)), dma((1,)), dma((4,)), dma((4,)), dma((4,)),
    ]
    anyspec = pl.BlockSpec(memory_space=pl.ANY)
    out_shape = tuple(
        jax.ShapeDtypeStruct(s, BF) for s in ((TD, FW), (FW // 16, HW), (FW // 16, HW), (HW // 16, FW))
    )
    results = pl.pallas_call(
        kernel,
        out_shape=out_shape,
        in_specs=[anyspec] * 5,
        out_specs=(anyspec,) * 4,
        scratch_shapes=scratch,
        compiler_params=pltpu.CompilerParams(
            collective_id=0, has_side_effects=True, vmem_limit_bytes=58 * 1024 * 1024
        ),
    )(tokens, w_gate, w_up, w_down, cotangent)
    return pl.pallas_call(
        written,
        out_shape=out_shape,
        in_specs=[anyspec] * 4,
        out_specs=(anyspec,) * 4,
        scratch_shapes=[pltpu.VMEM(o.shape, BF) for o in out_shape] + [dma((2, 4))],
    )(*results)


def solution(mesh):
    tok, grad = P(("col", "depth"), "row"), P(("row", "depth"), "col")
    return jax.shard_map(
        per_device,
        mesh=mesh,
        in_specs=(tok, P("row", "col"), P("row", "col"), P("col", "row"), tok),
        out_specs=(tok, grad, grad, P(("col", "depth"), "row")),
        check_vma=False,
    )
```
